32 devices in a mesh: ep: 8 (over z, y), dp: 4 (over x, core).
Axes of the slice: x: 2, y: 2, z: 4, core: 2. Of those that a mesh axis runs over, the one named last changes fastest.
Arguments:
- tokens: bfloat16 [4096, 7168], P(('dp', 'ep')), parts along dimension 0, may hold values from -18 to 18
- expert_ids: int32 [4096, 2], P(('dp', 'ep')), parts along dimension 0, may hold values from 0 to 3, all different within a row; in each aligned block of 128 rows (0 to 127, 128 to 255, ...) at most 128 rows name the same one
- affinity: float32 [4096, 2], P(('dp', 'ep')), parts along dimension 0, may hold values from 0.05 to 1
- w_gate: bfloat16 [8, 7168, 512], P('ep'), may hold values from -0.0625 to 0.0625
- w_up: bfloat16 [8, 7168, 512], P('ep'), may hold values from -0.0625 to 0.0625
- w_down: bfloat16 [8, 512, 7168], P('ep'), may hold values from -0.1875 to 0.1875
Outputs:
- mixed: bfloat16 [4096, 7168], P(('dp', 'ep')), parts along dimension 0
The draws below stay inside these ranges and needn't reach their ends.
There are 4 independent parts, one for each index of `dp`. The reference program is written for one: setup_inputs(seed, part) draws one part's arguments, and reference() takes and returns one part's arrays. A program takes and returns all parts, laid end to end along the dimension named above; an argument that names none is the same for every part. Nothing has to cross between parts.
Inputs may be any that keep to these rules, and one draw needn't show every extreme that they name: `expert_ids`: each row names 2 different experts; among the rows of one index of ep no expert is named by more than 128 rows.
All inputs are finite; a program needn't handle non-finite values.
Results may differ from the reference program's by a relative error of at most 0.019.
Values may be sent and summed in bfloat16 or wider, within the bound.
A program may use at most 256 MiB of HBM per device.

```python
import math
import jax
import jax.numpy as jnp
import numpy as np
from jax import lax

D = 7168
FF = 1024
TOP = 2
TOK_DEV = 128
FF_HALF = 512
EXPERTS = 4
CAP = 128
TOKENS = 1024
N_EP = 8


def draw_tokens(key, part):
    scale_key, block_key, value_key = jax.random.split(key, 3)
    row_scale = jnp.exp(jax.random.uniform(scale_key, (TOKENS, 1, 1), jnp.float32, jnp.log(0.8), jnp.log(1.25)))
    block_scale = jnp.exp(jax.random.uniform(block_key, (TOKENS, D // 16, 1), jnp.float32, jnp.log(0.05), jnp.log(2.0)))
    values = jnp.clip(jax.random.normal(value_key, (TOKENS, D // 16, 16), jnp.float32), -5.0, 5.0)
    return (values * block_scale * row_scale).reshape(TOKENS, D).astype(jnp.bfloat16)


def block_levels(own_key, shape, cuts, least, high):
    def one(dim, blocks):
        steps = jax.random.uniform(jax.random.fold_in(jax.random.fold_in(own_key, 6), dim), (blocks,), jnp.float32, least / len(cuts), high / len(cuts))
        return jnp.repeat(jnp.exp(steps), shape[dim] // blocks).reshape((-1,) + (1,) * (len(shape) - dim - 1))

    gain = one(*cuts[0])
    for cut in cuts[1:]:
        gain = gain * one(*cut)
    return gain


def deal_out(stream_key, own, number, rows, count, top, most, slope):
    ranking = jax.random.permutation(stream_key, count)
    crowded, usual = load_shares(count, rows * top, most, slope, True), load_shares(count, rows * top, most, slope, False)
    places = jnp.arange(count)

    def named(lengths, rotation):
        used = int((lengths > 0).sum())
        fixed = max(1, used // 4)
        passed = fixed + (places - fixed + rotation * (used - fixed)) % max(1, count - fixed)
        return jnp.zeros((count,), jnp.int32).at[ranking[jnp.where(places < fixed, places, passed)]].set(jnp.asarray(lengths, jnp.int32))

    lengths = jnp.where(number % 4 == 0, named(crowded, number // 4), named(usual, number - number // 4 - 1))
    mixed = jax.random.permutation(jax.random.fold_in(own, 3), count)
    donor, sink = mixed[0:count // 2 * 2:2], mixed[1:count // 2 * 2:2]
    room = jnp.minimum(lengths[donor] - 1, most - lengths[sink]) // 2
    room = jnp.where((donor == ranking[0]) | (sink == ranking[0]) | (lengths[sink] == 0), 0, jnp.maximum(room, 0))
    passed = jax.random.randint(jax.random.fold_in(own, 4), (count // 2,), 0, 1 << 20) % (room + 1)
    lengths = lengths.at[donor].add(-passed).at[sink].add(passed)
    labels = jnp.searchsorted(jnp.cumsum(lengths), jnp.arange(rows * top), side="right").astype(jnp.int32)
    grid = labels.reshape(top, rows).T
    grid = grid[jax.random.permutation(jax.random.fold_in(own, 1), rows)]
    rotation = jax.random.randint(jax.random.fold_in(own, 2), (rows, 1), 0, top)
    return jnp.take_along_axis(grid, (jnp.arange(top)[None, :] + rotation) % top, axis=1)


def load_shares(number_of, total, bound, lean, full):
    weights = [(1 << 20) // math.isqrt(standing ** lean) + 1 for standing in range(1, number_of + 1)]
    largest = bound if full else min(bound, max(-(-total // number_of), total * weights[0] // sum(weights)))
    least = 1 if total - largest >= number_of - 1 else 0
    counts, rest = [largest] + [least] * (number_of - 1), total - largest - least * (number_of - 1)
    while rest > 0:
        candidates = [i for i in range(1, number_of) if counts[i] < largest] or [i for i in range(1, number_of) if counts[i] < bound]
        mass, budget = sum([weights[i] for i in candidates]), rest
        for i in candidates:
            more = min(bound - counts[i], max(1, budget * weights[i] // mass), rest)
            counts[i] = counts[i] + more
            rest = rest - more
    return np.array(counts)


def noise(rng, extent, deviation, reach, cuts=(), kind=jnp.bfloat16):
    values = jax.random.normal(rng, extent, jnp.float32) * deviation
    if len(cuts) > 0:
        values = block_levels(rng, extent, cuts, -0.22, 0.18) * values
    return jnp.clip(values, min=-reach, max=reach).astype(kind)


def setup_inputs(seed: int = 0, part: int = 0) -> dict:
    streams_of = jax.random.split(jax.random.key(seed), 7)
    own_keys = jax.random.split(jax.random.fold_in(streams_of[6], part), 7)
    tokens = draw_tokens(jax.random.fold_in(jax.random.fold_in(streams_of[6], part), 71), part)
    expert_ids_keys = jax.random.split(jax.random.fold_in(own_keys[1], 1), TOKENS // TOK_DEV)
    expert_ids_turns = jax.random.permutation(jax.random.fold_in(own_keys[1], 3), TOKENS // TOK_DEV)
    expert_ids = jax.vmap(lambda own, number: deal_out(jax.random.fold_in(own_keys[1], 2), own, number, TOK_DEV, EXPERTS, TOP, CAP, 3))(expert_ids_keys, expert_ids_turns).reshape((TOKENS, TOP))
    affinity = jnp.clip(jnp.exp(math.log(1.0) - 2.9957323 * jax.random.uniform(own_keys[2], (TOKENS, TOP), jnp.float32) ** block_levels(own_keys[2], (TOKENS, TOP), ((0, 8),), -0.2, 0.2)), 0.05, 1.0)
    w_gate = noise(streams_of[3], (N_EP, D, FF_HALF), D ** -0.5, 0.0625, ((0, 8),))
    w_up = noise(streams_of[4], (N_EP, D, FF_HALF), D ** -0.5, 0.0625, ((0, 8),))
    w_down = noise(streams_of[5], (N_EP, FF_HALF, D), FF ** -0.5, 0.1875, ((0, 8),))
    return {"tokens": tokens, "expert_ids": expert_ids, "affinity": affinity, "w_gate": w_gate, "w_up": w_up, "w_down": w_down}


def quantize(tokens):
    count_rows = tokens.shape[0]
    blocks = tokens.astype(jnp.float32).reshape(count_rows, -1, 16)
    largest = jnp.max(jnp.abs(blocks), axis=2)
    scales = (jnp.maximum(largest, 0.25) / 9.0).astype(jnp.bfloat16)
    divided = blocks / scales.astype(jnp.float32)[:, :, None]
    payload = jnp.clip(divided, -6.0, 6.0).astype(jnp.bfloat16).reshape(count_rows, -1)
    return payload, scales


def restore(payload, scales):
    count_rows = payload.shape[0]
    values = payload.astype(jnp.float32).reshape(count_rows, -1, 16) * scales.astype(jnp.float32)[:, :, None]
    return values.astype(jnp.bfloat16).reshape(count_rows, -1)


def half_expert(restored, gate_half, up_half, down_half):
    gate = jnp.dot(restored, gate_half, preferred_element_type=jnp.float32)
    upward = jnp.dot(restored, up_half, preferred_element_type=jnp.float32)
    hidden = (jax.nn.silu(gate) * upward).astype(jnp.bfloat16)
    return jnp.dot(hidden, down_half, preferred_element_type=jnp.float32).astype(jnp.bfloat16)


def reference(tokens, expert_ids, affinity, w_gate, w_up, w_down):
    payload, scales = quantize(tokens)
    restored = restore(payload, scales)
    flat_ids = expert_ids.reshape(-1).astype(jnp.int32)
    assigned = flat_ids.shape[0]
    slot_total = N_EP * CAP

    def per_expert(expert):
        others = (flat_ids != expert).astype(jnp.int32)
        ordering = jnp.argsort(others, stable=True)[:slot_total].astype(jnp.int32)
        picked = restored[ordering // TOP]
        first_half = half_expert(picked, w_gate[2 * expert], w_up[2 * expert], w_down[2 * expert])
        second_half = half_expert(picked, w_gate[2 * expert + 1], w_up[2 * expert + 1], w_down[2 * expert + 1])
        summed = (first_half.astype(jnp.float32) + second_half.astype(jnp.float32)).astype(jnp.bfloat16)
        count_live = jnp.sum(1 - others)
        target_rows = jnp.where(jnp.arange(slot_total, dtype=jnp.int32) < count_live, ordering, assigned).astype(jnp.int32)
        return summed, target_rows

    outputs, targets = lax.map(per_expert, jnp.arange(EXPERTS, dtype=jnp.int32))
    per_slot = jnp.zeros((assigned, D), jnp.bfloat16).at[targets.reshape(-1)].set(outputs.reshape(-1, D), mode="drop")
    weights = affinity / jnp.sum(affinity, axis=1, keepdims=True)
    combined = jnp.sum(weights[:, :, None] * per_slot.astype(jnp.float32).reshape(TOKENS, TOP, D), axis=1)
    return combined.astype(jnp.bfloat16)
```

```python
import functools

import jax
import jax.numpy as jnp
from jax import lax
from jax.experimental import pallas as pl
from jax.experimental.pallas import tpu as pltpu
from jax.sharding import PartitionSpec as P

RING = 4
LANES = 128
MESH = pl.DeviceIdType.MESH
VMEM_LIMIT = 48 * 1024 * 1024


def requantized(tokens):
    rows, width = tokens.shape
    blocks = tokens.astype(jnp.float32).reshape(rows, -1, 16)
    largest = jnp.max(jnp.abs(blocks), axis=2)
    scales = (jnp.maximum(largest, 0.25) / 9.0).astype(jnp.bfloat16).astype(jnp.float32)
    divided = blocks / scales[:, :, None]
    payload = jnp.clip(divided, -6.0, 6.0).astype(jnp.bfloat16).astype(jnp.float32)
    return (payload * scales[:, :, None]).astype(jnp.bfloat16).reshape(rows, width)


def split_of(width):
    tiles = width // LANES
    return (tiles * 5 + 4) // 9 * LANES


def places():
    me = lax.axis_index("ep")
    z, y = me // 2, lax.rem(me, 2)
    up, down, far = lax.rem(z + 1, RING), lax.rem(z + 3, RING), lax.rem(z + 2, RING)
    return me, z, y, 1 - y, up, down, far


def meet(targets):
    barrier = pltpu.get_barrier_semaphore()
    for target in targets:
        pl.semaphore_signal(barrier, inc=1, device_id={"ep": target}, device_id_type=MESH)
    pl.semaphore_wait(barrier, len(targets))


def spread(n, x_ref, share_ref, all_ref, shares_ref, send, recv, local):
    me, z, y, other, up, down, far = places()
    rows, width = x_ref.shape
    cut = split_of(width)
    first, second = pl.ds(0, cut), pl.ds(cut, width - cut)
    upper, lower = pl.ds(0, rows // 2), pl.ds(rows // 2, rows // 2)
    full = pl.ds(0, rows)
    to_up, to_down, to_peer = 2 * up + y, 2 * down + y, 2 * z + other

    keep = pltpu.make_async_copy(x_ref, all_ref.at[me], local.at[0])
    keep_share = pltpu.make_async_copy(share_ref, shares_ref.at[me], local.at[1])
    keep.start()
    keep_share.start()
    meet([lax.rem(me + step, n) for step in range(1, n)])
    copies = {}

    def start(name, owner, rows_of, columns, target, own=False):
        k = len(copies)
        place = all_ref.at[owner, rows_of, columns]
        copies[name] = pltpu.make_async_remote_copy(
            src_ref=x_ref.at[rows_of, columns] if own else place,
            dst_ref=place,
            send_sem=send.at[k],
            recv_sem=recv.at[k],
            device_id={"ep": target},
            device_id_type=MESH,
        )
        copies[name].start()

    arrived = []

    def wait(name):
        copies[name].wait_recv()
        arrived.append(name)

    start("b_up", me, full, second, to_up, own=True)
    start("b_down", me, full, second, to_down, own=True)
    start("a_peer", me, full, first, to_peer, own=True)
    for step in range(1, n):
        k = len(copies)
        copies[("share", step)] = pltpu.make_async_remote_copy(
            src_ref=share_ref,
            dst_ref=shares_ref.at[me],
            send_sem=send.at[k],
            recv_sem=recv.at[k],
            device_id={"ep": lax.rem(me + step, n)},
            device_id_type=MESH,
        )
        copies[("share", step)].start()
    start("b_peer", me, full, second, to_peer, own=True)
    start("a_up", me, full, first, to_up, own=True)
    start("a_down", me, full, first, to_down, own=True)
    wait("b_up")
    start("b_up2", 2 * down + y, upper, second, to_up)
    start("b_up_peer", 2 * down + y, full, second, to_peer)
    wait("b_down")
    start("b_down2", 2 * up + y, lower, second, to_down)
    start("b_down_peer", 2 * up + y, full, second, to_peer)
    wait("a_peer")
    start("p_up", 2 * z + other, full, first, to_up)
    start("p_down", 2 * z + other, full, first, to_down)
    wait("a_up")
    start("a_up2", 2 * down + y, upper, first, to_up)
    wait("a_down")
    start("a_down2", 2 * up + y, lower, first, to_down)
    wait("b_up2")
    start("b_up2_peer", 2 * far + y, upper, second, to_peer)
    wait("b_down2")
    start("b_down2_peer", 2 * far + y, lower, second, to_peer)
    wait("p_up")
    start("p_up2", 2 * down + other, upper, first, to_up)
    wait("p_down")
    start("p_down2", 2 * up + other, lower, first, to_down)
    for name in list(copies):
        if name not in arrived:
            wait(name)
    for name in copies:
        copies[name].wait_send()
    keep.wait()
    keep_share.wait()


def all_tokens(restored, share):
    n = lax.axis_size("ep")
    rows, width = restored.shape
    count = 18 + n - 1
    return pl.pallas_call(
        functools.partial(spread, n),
        out_shape=(
            jax.ShapeDtypeStruct((n, rows, width), restored.dtype),
            jax.ShapeDtypeStruct((n,) + share.shape, share.dtype),
        ),
        in_specs=[pl.BlockSpec(memory_space=pltpu.VMEM)] * 2,
        out_specs=[pl.BlockSpec(memory_space=pl.ANY)] * 2,
        scratch_shapes=[
            pltpu.SemaphoreType.DMA((count,)),
            pltpu.SemaphoreType.DMA((count,)),
            pltpu.SemaphoreType.DMA((2,)),
        ],
        compiler_params=pltpu.CompilerParams(
            collective_id=0, has_side_effects=True, vmem_limit_bytes=VMEM_LIMIT
        ),
        name="spread",
    )(restored, share)


def add_up(target, sources):
    rows = target.shape[0]
    step = 16

    def body(i, carry):
        at = pl.ds(pl.multiple_of(i * step, step), step)
        total = sources[0][at, :].astype(jnp.float32)
        for source in sources[1:]:
            total = total + source[at, :].astype(jnp.float32)
        target[at, :] = total.astype(target.dtype)
        return carry

    lax.fori_loop(0, rows // step, body, 0)


def gather_sums(
    c_ref, out_ref, own_b, own_a, end_a, got_b, got_b1, got_b2, got_a1, got_a2, got_a3,
    send, recv, local,
):
    me, z, y, other, up, down, far = places()
    rows, width = out_ref.shape
    half = rows // 2
    cut = split_of(width)
    first, second = pl.ds(0, cut), pl.ds(cut, width - cut)
    full, upper, lower = pl.ds(0, rows), pl.ds(0, half), pl.ds(half, half)
    to_up, to_down, to_peer = 2 * up + y, 2 * down + y, 2 * z + other
    faces = (other, y)
    loads = {}
    copies = {}

    def load(name, owner, rows_of, columns, place):
        k = len(loads)
        loads[name] = pltpu.make_async_copy(
            c_ref.at[owner, rows_of, columns], place, local.at[k]
        )
        loads[name].start()

    def start(name, source, place, target):
        k = len(copies)
        copies[name] = pltpu.make_async_remote_copy(
            src_ref=source,
            dst_ref=place,
            send_sem=send.at[k],
            recv_sem=recv.at[k],
            device_id={"ep": target},
            device_id_type=MESH,
        )
        copies[name].start()

    def arrive(*names):
        for name in names:
            copies[name].wait_recv()

    for i in range(2):
        load(("a_up", i), 2 * up + faces[i], upper, first, own_a.at[0, i])
        load(("a_down", i), 2 * down + faces[i], lower, first, own_a.at[1, i])
    for i, place in enumerate((far, up, down, z)):
        load(("b", i), 2 * place + y, full, second, own_b.at[i])
    for i in range(2):
        load(("a", i), 2 * z + faces[i], full, first, end_a.at[i])
    meet([to_up, to_down, to_peer])
    start(("b", 0), c_ref.at[2 * far + other, full, second], got_b.at[0], to_peer)
    for i in range(2):
        owner = 2 * far + faces[i]
        start(("a1_up", i), c_ref.at[owner, upper, first], got_a1.at[0, i], to_up)
        start(("a1_down", i), c_ref.at[owner, lower, first], got_a1.at[1, i], to_down)
    for i, place in ((1, up), (2, down), (3, z)):
        start(("b", i), c_ref.at[2 * place + other, full, second], got_b.at[i], to_peer)
    for i in range(2):
        start(("r_up", i), c_ref.at[2 * up + faces[i], lower, first], got_a2.at[0, i, lower], to_up)
        start(("r_down", i), c_ref.at[2 * down + faces[i], upper, first], got_a2.at[1, i, upper], to_down)
    for name in loads:
        loads[name].wait()

    def pass_a(i):
        arrive(("a1_up", i))
        add_up(own_a.at[0, i], [own_a.at[0, i], got_a1.at[0, i]])
        start(("a2_up", i), own_a.at[0, i], got_a2.at[0, i, upper], to_up)
        arrive(("a1_down", i))
        add_up(own_a.at[1, i], [own_a.at[1, i], got_a1.at[1, i]])
        start(("a2_down", i), own_a.at[1, i], got_a2.at[1, i, lower], to_down)

    pass_a(0)
    arrive(("b", 0))
    add_up(own_b.at[0], [own_b.at[0], got_b.at[0]])
    start("b1_up", own_b.at[0, upper], got_b1.at[0], to_up)
    start("b1_down", own_b.at[0, lower], got_b1.at[1], to_down)
    pass_a(1)
    arrive(("b", 1), ("b", 2))
    add_up(own_b.at[1, lower], [own_b.at[1, lower], got_b.at[1, lower]])
    add_up(own_b.at[2, upper], [own_b.at[2, upper], got_b.at[2, upper]])
    arrive(("r_up", 0), ("r_down", 0), ("a2_up", 0), ("a2_down", 0))
    add_up(end_a.at[0], [end_a.at[0], got_a2.at[0, 0], got_a2.at[1, 0]])
    start("a3", end_a.at[0], got_a3, to_peer)
    arrive("b1_up")
    add_up(own_b.at[1, upper], [own_b.at[1, upper], got_b.at[1, upper], got_b1.at[0]])
    start("b2_up", own_b.at[1], got_b2.at[0], to_up)
    arrive("b1_down")
    add_up(own_b.at[2, lower], [own_b.at[2, lower], got_b.at[2, lower], got_b1.at[1]])
    start("b2_down", own_b.at[2], got_b2.at[1], to_down)
    arrive(("r_up", 1), ("r_down", 1), ("a2_up", 1), ("a2_down", 1))
    arrive(("b", 3), "a3")
    add_up(out_ref.at[:, first], [end_a.at[1], got_a2.at[0, 1], got_a2.at[1, 1], got_a3])
    arrive("b2_up", "b2_down")
    add_up(out_ref.at[:, second], [own_b.at[3], got_b.at[3], got_b2.at[0], got_b2.at[1]])
    for name in copies:
        copies[name].wait_send()


def summed(scaled):
    n, rows, width = scaled.shape
    half = rows // 2
    cut = split_of(width)
    rest = width - cut
    kind = scaled.dtype
    return pl.pallas_call(
        gather_sums,
        out_shape=jax.ShapeDtypeStruct((rows, width), kind),
        in_specs=[pl.BlockSpec(memory_space=pl.ANY)],
        out_specs=pl.BlockSpec(memory_space=pltpu.VMEM),
        scratch_shapes=[
            pltpu.VMEM((4, rows, rest), kind),
            pltpu.VMEM((2, 2, half, cut), kind),
            pltpu.VMEM((2, rows, cut), kind),
            pltpu.VMEM((4, rows, rest), kind),
            pltpu.VMEM((2, half, rest), kind),
            pltpu.VMEM((2, rows, rest), kind),
            pltpu.VMEM((2, 2, half, cut), kind),
            pltpu.VMEM((2, 2, rows, cut), kind),
            pltpu.VMEM((rows, cut), kind),
            pltpu.SemaphoreType.DMA((21,)),
            pltpu.SemaphoreType.DMA((21,)),
            pltpu.SemaphoreType.DMA((10,)),
        ],
        compiler_params=pltpu.CompilerParams(
            collective_id=1, has_side_effects=True, vmem_limit_bytes=VMEM_LIMIT
        ),
        name="gather_sums",
    )(scaled)


def on_device(tokens, expert_ids, affinity, w_gate, w_up, w_down):
    n = lax.axis_size("ep")
    experts = n // 2
    own = lax.axis_index("ep") // 2
    rows, width = tokens.shape
    restored = requantized(tokens)
    weights = affinity / jnp.sum(affinity, axis=1, keepdims=True)
    padded = -(-experts // 8) * 8
    names = jnp.arange(padded, dtype=jnp.int32)[:, None]
    shares = sum(
        jnp.where(expert_ids[:, k][None, :] == names, weights[:, k][None, :], 0.0)
        for k in range(weights.shape[1])
    )
    by_ring = experts == RING and rows % 32 == 0 and width % LANES == 0
    if by_ring:
        every, shares = all_tokens(restored, shares)
    else:
        every = lax.all_gather(restored, "ep", axis=0, tiled=False)
        shares = lax.all_gather(shares, "ep", axis=0, tiled=False)
    every = every.reshape(n * rows, width)
    share = lax.dynamic_slice_in_dim(shares, own, 1, axis=1).reshape(n * rows, 1)
    gate = jnp.dot(every, w_gate[0], preferred_element_type=jnp.float32)
    upward = jnp.dot(every, w_up[0], preferred_element_type=jnp.float32)
    hidden = (jax.nn.silu(gate) * upward).astype(jnp.bfloat16)
    partial = jnp.dot(hidden, w_down[0], preferred_element_type=jnp.float32)
    scaled = (partial * share).astype(jnp.bfloat16)
    if by_ring:
        return summed(scaled.reshape(n, rows, width))
    return lax.psum_scatter(scaled, "ep", scatter_dimension=0, tiled=True)


def solution(mesh):
    in_specs = (
        P(("dp", "ep"), None),
        P(("dp", "ep"), None),
        P(("dp", "ep"), None),
        P("ep", None, None),
        P("ep", None, None),
        P("ep", None, None),
    )
    return jax.shard_map(
        on_device, mesh=mesh, in_specs=in_specs, out_specs=P(("dp", "ep"), None), check_vma=False
    )
```

```python
import functools

import jax
import jax.numpy as jnp
from jax import lax
from jax.experimental import pallas as pl
from jax.experimental.pallas import tpu as pltpu
from jax.sharding import PartitionSpec as P

LINE = 4
LANES = 128
MESH = pl.DeviceIdType.MESH
VMEM_LIMIT = 48 * 1024 * 1024


def requantized(tokens):
    rows, width = tokens.shape
    blocks = tokens.astype(jnp.float32).reshape(rows, -1, 16)
    largest = jnp.max(jnp.abs(blocks), axis=2)
    scales = (jnp.maximum(largest, 0.25) / 9.0).astype(jnp.bfloat16).astype(jnp.float32)
    divided = blocks / scales[:, :, None]
    payload = jnp.clip(divided, -6.0, 6.0).astype(jnp.bfloat16).astype(jnp.float32)
    return (payload * scales[:, :, None]).astype(jnp.bfloat16).reshape(rows, width)


def split_of(width):
    return width // LANES // 6 * LANES


def halves_of(rows):
    return pl.ds(0, rows // 2), pl.ds(rows // 2, rows // 2)


def meet(targets):
    barrier = pltpu.get_barrier_semaphore()
    for target in targets:
        pl.semaphore_signal(barrier, inc=1, device_id={"ep": target}, device_id_type=MESH)
    pl.semaphore_wait(barrier, len(targets))


def swap(values, lane, distance):
    high = (lane // distance) % 2 == 1
    width = values.shape[1]
    return jnp.where(
        high, pltpu.roll(values, distance, 1), pltpu.roll(values, width - distance, 1)
    )


def quantize_into(tokens_ref, x_ref):
    rows, width = x_ref.shape

    def body(i, carry):
        at = pl.ds(pl.multiple_of(i * LANES, LANES), LANES)
        values = tokens_ref[:, at].astype(jnp.float32)
        lane = lax.broadcasted_iota(jnp.int32, values.shape, 1)
        largest = jnp.abs(values)
        for distance in (1, 2, 4, 8):
            largest = jnp.maximum(largest, swap(largest, lane, distance))
        scales = (jnp.maximum(largest, 0.25) / 9.0).astype(jnp.bfloat16).astype(jnp.float32)
        payload = jnp.clip(values / scales, -6.0, 6.0).astype(jnp.bfloat16).astype(jnp.float32)
        x_ref[:, at] = (payload * scales).astype(x_ref.dtype)
        return carry

    lax.fori_loop(0, width // LANES, body, 0)


class Copies:
    def __init__(self, send, recv):
        self.send, self.recv, self.numbers = send, recv, {}

    def number(self, name):
        return self.numbers.setdefault(name, len(self.numbers))

    def make(self, name, source, place, target):
        k = self.number(name)
        return pltpu.make_async_remote_copy(
            src_ref=source,
            dst_ref=place,
            send_sem=self.send.at[k],
            recv_sem=self.recv.at[k],
            device_id={"ep": target},
            device_id_type=MESH,
        )


def spread(n, tokens_ref, share_ref, all_ref, shares_ref, x_ref, send, recv, local):
    me = lax.axis_index("ep")
    here, y = me // 2, lax.rem(me, 2)
    other = 1 - y
    peer = 2 * here + other
    rows, width = x_ref.shape
    cut = split_of(width)
    first, second = pl.ds(0, cut), pl.ds(cut, width - cut)
    full, halves = pl.ds(0, rows), halves_of(rows)
    quantize_into(tokens_ref, x_ref)
    keep = pltpu.make_async_copy(x_ref, all_ref.at[me], local.at[0])
    keep_share = pltpu.make_async_copy(share_ref, shares_ref.at[me], local.at[1])
    keep.start()
    keep_share.start()
    meet([lax.rem(me + step, n) for step in range(1, n)])
    all_copies = Copies(send, recv)
    shares = [
        all_copies.make(("share", step), share_ref, shares_ref.at[me], lax.rem(me + step, n))
        for step in range(1, n)
    ]
    last = LINE - 1

    def program(z):
        started = []

        def block(owner, side, rows_of, columns):
            return all_ref.at[2 * owner + side, rows_of, columns]

        def start(name, owner, side, rows_of, columns, target, own=False):
            place = block(owner, side, rows_of, columns)
            source = x_ref.at[rows_of, columns] if own else place
            copy = all_copies.make(name, source, place, target)
            copy.start()
            started.append(copy)

        def wait(name, owner, side, rows_of, columns):
            place = block(owner, side, rows_of, columns)
            all_copies.make(name, place, place, peer).wait_recv()

        def onward(kind, owner, side, rows_of, columns, source_z, own=False):
            for way, ok, step in (("up", z < last, 1), ("down", z > 0, -1)):
                if ok and (source_z - z) * step <= 0:
                    start((kind, way, owner), owner, side, rows_of, columns, 2 * (z + step) + y, own)

        def way_of(owner):
            return "up" if owner < z else "down"

        def pass_b(owner, i):
            own = owner == z
            if not own:
                wait((("b", i), way_of(owner), owner), owner, y, halves[i], second)
            onward(("b", i), owner, y, halves[i], second, owner, own)
            start((("b", i), "peer", owner), owner, y, halves[i], second, peer, own)

        def pass_a(kind, owner, side):
            wait((kind, way_of(owner), owner), owner, side, full, first)
            onward(kind, owner, side, full, first, owner)

        start(("a", "peer"), z, y, full, first, peer, True)
        pass_b(z, 0)
        for copy in shares:
            copy.start()
        pass_b(z, 1)
        onward("a", z, y, full, first, z, True)
        by_distance = [
            [owner for owner in (z - hop, z + hop) if 0 <= owner <= last] for hop in range(1, LINE)
        ]
        for hop in range(LINE - 1):
            for i in range(2):
                for owner in by_distance[hop]:
                    pass_b(owner, i)
            if hop == 1:
                wait(("a", "peer"), z, other, full, first)
                onward("p", z, other, full, first, z)
        for owners in by_distance:
            for owner in owners:
                pass_a("a", owner, y)
            for owner in owners:
                pass_a("p", owner, other)
        for owner in range(LINE):
            for i in range(2):
                wait((("b", i), "peer", owner), owner, other, halves[i], second)
        for copy in started:
            copy.wait_send()

    for z in range(LINE):
        pl.when(here == z)(functools.partial(program, z))
    for copy in shares:
        copy.wait()
    keep.wait()
    keep_share.wait()


def all_tokens(tokens, share):
    n = lax.axis_size("ep")
    rows, width = tokens.shape
    count = 64
    return pl.pallas_call(
        functools.partial(spread, n),
        out_shape=(
            jax.ShapeDtypeStruct((n, rows, width), tokens.dtype),
            jax.ShapeDtypeStruct((n,) + share.shape, share.dtype),
        ),
        in_specs=[pl.BlockSpec(memory_space=pltpu.VMEM)] * 2,
        out_specs=[pl.BlockSpec(memory_space=pl.ANY)] * 2,
        scratch_shapes=[
            pltpu.VMEM((rows, width), tokens.dtype),
            pltpu.SemaphoreType.DMA((count,)),
            pltpu.SemaphoreType.DMA((count,)),
            pltpu.SemaphoreType.DMA((2,)),
        ],
        compiler_params=pltpu.CompilerParams(
            collective_id=0, has_side_effects=True, vmem_limit_bytes=VMEM_LIMIT
        ),
        name="spread",
    )(tokens, share)


def add_up(target, sources):
    rows = target.shape[0]
    step = 16

    def body(i, carry):
        at = pl.ds(pl.multiple_of(i * step, step), step)
        total = sources[0][at, :].astype(jnp.float32)
        for source in sources[1:]:
            total = total + source[at, :].astype(jnp.float32)
        target[at, :] = total.astype(target.dtype)
        return carry

    lax.fori_loop(0, rows // step, body, 0)


def gather_sums(
    c_ref, out_ref, own_b, own_a, got_b, zed_b, zed_a, got_a3, send, recv, local
):
    me = lax.axis_index("ep")
    here, y = me // 2, lax.rem(me, 2)
    other = 1 - y
    peer = 2 * here + other
    rows, width = out_ref.shape
    cut = split_of(width)
    first, second = pl.ds(0, cut), pl.ds(cut, width - cut)
    halves = halves_of(rows)
    faces = (other, y)
    last = LINE - 1
    loads = []

    def load(owner, columns, place):
        k = len(loads)
        loads.append(pltpu.make_async_copy(c_ref.at[owner, :, columns], place, local.at[k]))
        loads[k].start()

    for d in range(LINE):
        for i in range(2):
            load(2 * d + faces[i], first, own_a.at[d, i])
    for d in range(LINE):
        load(2 * d + y, second, own_b.at[d])
    meet([lax.rem(me + step, 2 * LINE) for step in range(1, 2 * LINE)])
    all_copies = Copies(send, recv)

    def program(z):
        started = []
        if z in (0, last):
            order = sorted((d for d in range(LINE) if d != z), key=lambda d: -abs(d - z))
        else:
            far, near = (last, 0) if z < last - z else (0, last)
            order = [far, near] + [d for d in range(1, last) if d != z]

        def send_off(name, source, place, target):
            copy = all_copies.make(name, source, place, target)
            copy.start()
            started.append(copy)

        def wait(name, place):
            all_copies.make(name, place, place, peer).wait_recv()

        def feeders(d):
            found = []
            if z > 0 and d >= z:
                found.append(0)
            if z < last and d <= z:
                found.append(1)
            return found

        def take_a(d, i):
            found = feeders(d)
            for way in found:
                wait(("a", way, d, i), zed_a.at[way, d, i])
            return [zed_a.at[way, d, i] for way in found]

        def take_b(d, h):
            wait(("y", d, h), got_b.at[d, halves[h]])
            found = feeders(d)
            for way in found:
                wait(("b", way, d, h), zed_b.at[way, d, halves[h]])
            return [got_b.at[d, halves[h]]] + [zed_b.at[way, d, halves[h]] for way in found]

        def pass_a(d):
            way, target = (0, 2 * (z + 1) + y) if d > z else (1, 2 * (z - 1) + y)
            for i in range(2):
                sources = take_a(d, i)
                if sources:
                    add_up(own_a.at[d, i], [own_a.at[d, i]] + sources)
                send_off(("a", way, d, i), own_a.at[d, i], zed_a.at[way, d, i], target)

        def pass_b(d):
            way, target = (0, 2 * (z + 1) + y) if d > z else (1, 2 * (z - 1) + y)
            for h in range(2):
                mine = own_b.at[d, halves[h]]
                add_up(mine, [mine] + take_b(d, h))
                send_off(("b", way, d, h), mine, zed_b.at[way, d, halves[h]], target)

        for d in order + [z]:
            for h in range(2):
                send_off(
                    ("y", d, h),
                    c_ref.at[2 * d + other, halves[h], second],
                    got_b.at[d, halves[h]],
                    peer,
                )
        for copy in loads:
            copy.wait()
        for d in order:
            pass_a(d)
        rest = order
        if z in (0, last):
            pass_b(order[0])
            rest = order[1:]
        add_up(own_a.at[z, 0], [own_a.at[z, 0]] + take_a(z, 0))
        send_off("a3", own_a.at[z, 0], got_a3, peer)
        ends = take_a(z, 1)
        for d in rest:
            pass_b(d)
        for h in range(2):
            add_up(out_ref.at[halves[h], second], [own_b.at[z, halves[h]]] + take_b(z, h))
        wait("a3", got_a3)
        add_up(out_ref.at[:, first], [own_a.at[z, 1], got_a3] + ends)
        for copy in started:
            copy.wait_send()

    for z in range(LINE):
        pl.when(here == z)(functools.partial(program, z))


def summed(scaled):
    n, rows, width = scaled.shape
    cut = split_of(width)
    rest = width - cut
    kind = scaled.dtype
    count = 48
    return pl.pallas_call(
        gather_sums,
        out_shape=jax.ShapeDtypeStruct((rows, width), kind),
        in_specs=[pl.BlockSpec(memory_space=pl.ANY)],
        out_specs=pl.BlockSpec(memory_space=pltpu.VMEM),
        scratch_shapes=[
            pltpu.VMEM((LINE, rows, rest), kind),
            pltpu.VMEM((LINE, 2, rows, cut), kind),
            pltpu.VMEM((LINE, rows, rest), kind),
            pltpu.VMEM((2, LINE, rows, rest), kind),
            pltpu.VMEM((2, LINE, 2, rows, cut), kind),
            pltpu.VMEM((rows, cut), kind),
            pltpu.SemaphoreType.DMA((count,)),
            pltpu.SemaphoreType.DMA((count,)),
            pltpu.SemaphoreType.DMA((3 * LINE,)),
        ],
        compiler_params=pltpu.CompilerParams(
            collective_id=1, has_side_effects=True, vmem_limit_bytes=VMEM_LIMIT
        ),
        name="gather_sums",
    )(scaled)


def on_device(tokens, expert_ids, affinity, w_gate, w_up, w_down):
    n = lax.axis_size("ep")
    experts = n // 2
    own = lax.axis_index("ep") // 2
    rows, width = tokens.shape
    weights = affinity / jnp.sum(affinity, axis=1, keepdims=True)
    padded = -(-experts // 8) * 8
    names = jnp.arange(padded, dtype=jnp.int32)[:, None]
    shares = sum(
        jnp.where(expert_ids[:, k][None, :] == names, weights[:, k][None, :], 0.0)
        for k in range(weights.shape[1])
    )
    by_line = experts == LINE and rows % 32 == 0 and width % LANES == 0
    if by_line:
        every, shares = all_tokens(tokens, shares)
    else:
        every = lax.all_gather(requantized(tokens), "ep", axis=0, tiled=False)
        shares = lax.all_gather(shares, "ep", axis=0, tiled=False)
    every = every.reshape(n * rows, width)
    share = lax.dynamic_slice_in_dim(shares, own, 1, axis=1).reshape(n * rows, 1)
    gate = jnp.dot(every, w_gate[0], preferred_element_type=jnp.float32)
    upward = jnp.dot(every, w_up[0], preferred_element_type=jnp.float32)
    hidden = (jax.nn.silu(gate) * upward).astype(jnp.bfloat16)
    partial = jnp.dot(hidden, w_down[0], preferred_element_type=jnp.float32)
    scaled = (partial * share).astype(jnp.bfloat16)
    if by_line:
        return summed(scaled.reshape(n, rows, width))
    return lax.psum_scatter(scaled, "ep", scatter_dimension=0, tiled=True)


def solution(mesh):
    in_specs = (
        P(("dp", "ep"), None),
        P(("dp", "ep"), None),
        P(("dp", "ep"), None),
        P("ep", None, None),
        P("ep", None, None),
        P("ep", None, None),
    )
    return jax.shard_map(
        on_device, mesh=mesh, in_specs=in_specs, out_specs=P(("dp", "ep"), None), check_vma=False
    )
```
